32 devices in a mesh: batch: 8 (over z, y), group: 4 (over x, core).
Axes of the slice: x: 2, y: 2, z: 4, core: 2. Of those that a mesh axis runs over, the one named last changes fastest.
Arguments:
- samples_in: float32 [2048, 1024], P('batch', 'group'), may hold values from -8 to 8, as said below
- second_samples_in: float32 [2048, 1024], P('batch', 'group'), may hold values from -8 to 8, as said below
Outputs:
- standard: float32 [2048, 1024], P(None, ('group', 'batch'))
- second_standard: float32 [2048, 1024], P(None, ('group', 'batch'))
The draws below stay inside these ranges and needn't reach their ends.
Inputs may be any that keep to these rules, and one draw needn't show every extreme that they name: samples_in holds numbers from -8 to 8. second_samples_in holds numbers from -8 to 8.
All inputs are finite; a program needn't handle non-finite values.
Results may differ from the reference program's by a relative error of at most 0.0003.
Values sent between devices are 32-bit elements.
A program may use at most 64 MiB of HBM per device.

```python
import jax
import jax.numpy as jnp

ROW_DEV = 256
ROWS = 2048
COLS = 1024
N_BATCH = 8


def column_values(key, tag):
    keys = jax.random.split(jax.random.fold_in(key, tag), 4)
    level = jax.random.normal(keys[0], (1, 1, COLS), jnp.float32) * 1.0
    spread = jnp.exp(jax.random.uniform(keys[1], (1, 1, COLS), jnp.float32, -0.7, 0.7))
    drift = jax.random.normal(keys[2], (N_BATCH, 1, COLS), jnp.float32) * 1.0
    noise = jax.random.normal(keys[3], (N_BATCH, ROW_DEV, COLS), jnp.float32) * 0.6
    return level + spread * (drift + noise)


def draw_samples_in(key, part):
    values = column_values(key, 1)
    return jnp.clip(values, -8.0, 8.0).reshape(ROWS, COLS)


def draw_second_samples_in(key, part):
    values = column_values(key, 2)
    return jnp.clip(values, -8.0, 8.0).reshape(ROWS, COLS)


def setup_inputs(seed: int = 0) -> dict:
    key_list = jax.random.split(jax.random.key(seed), 3)
    return {
        "samples_in": draw_samples_in(jax.random.fold_in(key_list[2], 71), 0),
        "second_samples_in": draw_second_samples_in(jax.random.fold_in(key_list[2], 71), 0),
    }


def reference(samples_in, second_samples_in):
    wide_standard = samples_in.astype(jnp.float32)
    low_standard = jnp.mean(jnp.minimum(wide_standard, 1.0), axis=0)
    high_standard = jnp.mean(jnp.maximum(wide_standard, 1.0), axis=0)
    standard = ((wide_standard - low_standard) / (high_standard - low_standard + 0.1))
    wide_second_standard = second_samples_in.astype(jnp.float32)
    low_second_standard = jnp.mean(jnp.minimum(wide_second_standard, 1.0), axis=0)
    high_second_standard = jnp.mean(jnp.maximum(wide_second_standard, 1.0), axis=0)
    second_standard = ((wide_second_standard - low_second_standard) / (high_second_standard - low_second_standard + 0.1))
    return standard, second_standard
```

```python
import functools

import jax
import jax.numpy as jnp
from jax import lax
from jax.experimental import pallas as pl
from jax.experimental.pallas import tpu as pltpu
from jax.sharding import PartitionSpec as P

MESH = pl.DeviceIdType.MESH
LANES = 128


def loop(count, body, init):
    if count <= 8:
        for step in range(count):
            init = body(step, init)
        return init
    return lax.fori_loop(0, count, body, init)


def kernel(n, first_hbm, second_hbm, first_out, second_out, raw, turned, got, load_sem, send_sem, recv_sem):
    ins = (first_hbm, second_hbm)
    outs = (first_out, second_out)
    rows, width = first_hbm.shape
    block = width // n
    half = n // 2
    span = half * block
    me = lax.axis_index("batch")
    mine, place = me // half, me % half
    sides = ((mine + 1) % 2, mine)

    def load(side, a):
        start = pl.multiple_of(sides[side] * span, span)
        return pltpu.make_async_copy(
            ins[a].at[:, pl.ds(start, span)], raw.at[a, side], load_sem.at[a, side]
        )

    for side in range(2):
        for a in range(2):
            load(side, a).start()

    barrier = pltpu.get_barrier_semaphore()

    def greet(step, carry):
        pl.semaphore_signal(
            barrier, inc=1, device_id={"batch": (me + 1 + step) % n}, device_id_type=MESH
        )
        return carry

    loop(n - 1, greet, 0)

    def send(side, a, step):
        spot = (place + step) % half
        return pltpu.make_async_remote_copy(
            src_ref=turned.at[a, side, spot],
            dst_ref=got.at[a, me],
            send_sem=send_sem.at[a, side, step],
            recv_sem=recv_sem.at[a, me],
            device_id={"batch": sides[side] * half + spot},
            device_id_type=MESH,
        )

    def arrival(side, a, step):
        source = sides[side] * half + (place - step + half) % half
        copy = pltpu.make_async_remote_copy(
            src_ref=turned.at[a, side, 0],
            dst_ref=got.at[a, source],
            send_sem=send_sem.at[a, side, step],
            recv_sem=recv_sem.at[a, source],
            device_id={"batch": source},
            device_id_type=MESH,
        )
        return source, copy

    greeted = False
    for side in range(2):
        for a in range(2):
            load(side, a).wait()
            for start in range(0, span, LANES):
                tile = raw[a, side, :, start : start + LANES].T
                turned[a, side, start // block : (start + LANES) // block] = tile.reshape(
                    LANES // block, block, rows
                )
            if not greeted:
                pl.semaphore_wait(barrier, n - 1)
                greeted = True

            def push(step, carry, side=side, a=a):
                send(side, a, step + side).start()
                return carry

            loop(half - side, push, 0)

    def add(sums, values):
        low, high = sums
        for start in range(0, rows, LANES):
            part = values[:, start : start + LANES]
            low += jnp.minimum(part, 1.0)
            high += jnp.maximum(part, 1.0)
        return low, high

    zero = jnp.zeros((block, LANES), jnp.float32)
    sums = []
    for a in range(2):
        own = turned[a, 1, place]
        got[a, me] = own
        sums.append(add((zero, zero), own))
    for side in range(2):
        for a in range(2):

            def take(step, carry, side=side, a=a):
                source, copy = arrival(side, a, step + side)
                copy.wait_recv()
                return add(carry, got[a, source])

            sums[a] = loop(half - side, take, sums[a])

    for a in range(2):
        low, high = (jnp.sum(s, axis=1, keepdims=True) / (n * rows) for s in sums[a])
        scale = 1.0 / (high - low + 0.1)
        low = jnp.broadcast_to(low, (block, rows))
        scale = jnp.broadcast_to(scale, (block, rows))
        out = outs[a]

        def rescale(source, carry, a=a, out=out, low=low, scale=scale):
            start = source * rows
            if not isinstance(start, int):
                start = pl.multiple_of(start, LANES)
            out[:, pl.ds(start, rows)] = (got[a, source] - low) * scale
            return carry

        loop(n, rescale, 0)

    for side in range(2):
        for a in range(2):

            def drain(step, carry, side=side, a=a):
                send(side, a, step + side).wait_send()
                return carry

            loop(half - side, drain, 0)


def solution(mesh):
    n = mesh.shape["batch"]

    def shards(samples_in, second_samples_in):
        rows, width = samples_in.shape
        block = width // n
        half = n // 2
        out = jax.ShapeDtypeStruct((block, n * rows), jnp.float32)
        first, second = pl.pallas_call(
            functools.partial(kernel, n),
            out_shape=(out, out),
            in_specs=[pl.BlockSpec(memory_space=pl.ANY)] * 2,
            out_specs=[pl.BlockSpec(memory_space=pltpu.VMEM)] * 2,
            scratch_shapes=[
                pltpu.VMEM((2, 2, rows, half * block), jnp.float32),
                pltpu.VMEM((2, 2, half, block, rows), jnp.float32),
                pltpu.VMEM((2, n, block, rows), jnp.float32),
                pltpu.SemaphoreType.DMA((2, 2)),
                pltpu.SemaphoreType.DMA((2, 2, half)),
                pltpu.SemaphoreType.DMA((2, n)),
            ],
            compiler_params=pltpu.CompilerParams(collective_id=0, has_side_effects=True),
            name="exchange",
        )(samples_in, second_samples_in)
        return first.T, second.T

    placed = (P("batch", "group"), P("batch", "group"))
    return jax.shard_map(
        shards,
        mesh=mesh,
        in_specs=placed,
        out_specs=(P(None, ("group", "batch")), P(None, ("group", "batch"))),
        check_vma=False,
    )
```

```python
import functools

import jax
import jax.numpy as jnp
from jax import lax
from jax.experimental import pallas as pl
from jax.experimental.pallas import tpu as pltpu
from jax.sharding import PartitionSpec as P

MESH = pl.DeviceIdType.MESH
LANES = 128


def loop(count, body, init):
    if count <= 8:
        for step in range(count):
            init = body(step, init)
        return init
    return lax.fori_loop(0, count, body, init)


def kernel(n, first_hbm, second_hbm, got, total, raw, turned, load_sem, send_sem, recv_sem):
    ins = (first_hbm, second_hbm)
    rows, width = first_hbm.shape
    block = width // n
    half = n // 2
    span = half * block
    me = lax.axis_index("batch")
    mine, place = me // half, me % half
    sides = ((mine + 1) % 2, mine)

    def load(side, a):
        start = pl.multiple_of(sides[side] * span, span)
        return pltpu.make_async_copy(
            ins[a].at[:, pl.ds(start, span)], raw.at[a, side], load_sem.at[a, side]
        )

    for side in range(2):
        for a in range(2):
            load(side, a).start()

    barrier = pltpu.get_barrier_semaphore()

    def greet(step, carry):
        pl.semaphore_signal(
            barrier, inc=1, device_id={"batch": (me + 1 + step) % n}, device_id_type=MESH
        )
        return carry

    loop(n - 1, greet, 0)

    def send(side, a, step):
        spot = (place + step) % half
        return pltpu.make_async_remote_copy(
            src_ref=turned.at[a, side, spot],
            dst_ref=got.at[a, me],
            send_sem=send_sem.at[a, side, step],
            recv_sem=recv_sem.at[a, me],
            device_id={"batch": sides[side] * half + spot},
            device_id_type=MESH,
        )

    def arrival(side, a, step):
        source = sides[side] * half + (place - step + half) % half
        copy = pltpu.make_async_remote_copy(
            src_ref=turned.at[a, side, 0],
            dst_ref=got.at[a, source],
            send_sem=send_sem.at[a, side, step],
            recv_sem=recv_sem.at[a, source],
            device_id={"batch": source},
            device_id_type=MESH,
        )
        return source, copy

    greeted = False
    for side in range(2):
        for a in range(2):
            load(side, a).wait()
            for start in range(0, span, LANES):
                tile = raw[a, side, :, start : start + LANES].T
                turned[a, side, start // block : (start + LANES) // block] = tile.reshape(
                    LANES // block, block, rows
                )
            if not greeted:
                pl.semaphore_wait(barrier, n - 1)
                greeted = True

            def push(step, carry, side=side, a=a):
                send(side, a, step + side).start()
                return carry

            loop(half - side, push, 0)

    def add(sums, values):
        low, high = sums
        for start in range(0, rows, LANES):
            part = values[:, start : start + LANES]
            low += jnp.minimum(part, 1.0)
            high += jnp.maximum(part, 1.0)
        return low, high

    zero = jnp.zeros((block, LANES), jnp.float32)
    sums = []
    for a in range(2):
        own = turned[a, 1, place]
        got[a, me] = own
        sums.append(add((zero, zero), own))
    for side in range(2):
        for a in range(2):

            def take(step, carry, side=side, a=a):
                source, copy = arrival(side, a, step + side)
                copy.wait_recv()
                return add(carry, got[a, source])

            sums[a] = loop(half - side, take, sums[a])

    for a in range(2):
        for kind in range(2):
            total[a, kind] = sums[a][kind]

    for side in range(2):
        for a in range(2):

            def drain(step, carry, side=side, a=a):
                send(side, a, step + side).wait_send()
                return carry

            loop(half - side, drain, 0)


def rescale(got, total, first_out, second_out, ready, store_sem):
    _, n, block, rows = got.shape
    outs = (first_out, second_out)
    pieces = min(n, 4)
    each = n // pieces
    copies = []
    for a in range(2):
        low, high = (
            jnp.sum(total[a, kind], axis=1, keepdims=True) / (n * rows) for kind in range(2)
        )
        scale = 1.0 / (high - low + 0.1)
        low = jnp.broadcast_to(low, (block, rows))
        scale = jnp.broadcast_to(scale, (block, rows))
        for piece in range(pieces):

            def turn(step, carry, a=a, piece=piece, low=low, scale=scale):
                source = piece * each + step
                start = source * rows
                if not isinstance(start, int):
                    start = pl.multiple_of(start, LANES)
                ready[a, :, pl.ds(start, rows)] = (got[a, source] - low) * scale
                return carry

            loop(each, turn, 0)
            part = pl.ds(piece * each * rows, each * rows)
            copy = pltpu.make_async_copy(
                ready.at[a, :, part], outs[a].at[:, part], store_sem.at[a, piece]
            )
            copy.start()
            copies.append(copy)
    for copy in copies:
        copy.wait()


def solution(mesh):
    n = mesh.shape["batch"]

    def shards(samples_in, second_samples_in):
        rows, width = samples_in.shape
        block = width // n
        half = n // 2
        held = 2 * rows * width * 4
        got, total = pl.pallas_call(
            functools.partial(kernel, n),
            out_shape=(
                pltpu.VMEM((2, n, block, rows), jnp.float32),
                pltpu.VMEM((2, 2, block, LANES), jnp.float32),
            ),
            in_specs=[pl.BlockSpec(memory_space=pltpu.HBM)] * 2,
            out_specs=[pl.BlockSpec(memory_space=pltpu.VMEM)] * 2,
            scratch_shapes=[
                pltpu.VMEM((2, 2, rows, half * block), jnp.float32),
                pltpu.VMEM((2, 2, half, block, rows), jnp.float32),
                pltpu.SemaphoreType.DMA((2, 2)),
                pltpu.SemaphoreType.DMA((2, 2, half)),
                pltpu.SemaphoreType.DMA((2, n)),
            ],
            compiler_params=pltpu.CompilerParams(
                collective_id=0, has_side_effects=True, vmem_limit_bytes=4 * held + (8 << 20)
            ),
            name="exchange",
        )(
            pltpu.with_memory_space_constraint(samples_in, pltpu.HBM),
            pltpu.with_memory_space_constraint(second_samples_in, pltpu.HBM),
        )
        out = jax.ShapeDtypeStruct((block, n * rows), jnp.float32)
        first, second = pl.pallas_call(
            rescale,
            out_shape=(out, out),
            in_specs=[pl.BlockSpec(memory_space=pltpu.VMEM)] * 2,
            out_specs=[pl.BlockSpec(memory_space=pl.ANY)] * 2,
            scratch_shapes=[
                pltpu.VMEM((2, block, n * rows), jnp.float32),
                pltpu.SemaphoreType.DMA((2, min(n, 4))),
            ],
            compiler_params=pltpu.CompilerParams(vmem_limit_bytes=2 * held + (8 << 20)),
            name="rescale",
        )(
            pltpu.with_memory_space_constraint(got, pltpu.VMEM),
            pltpu.with_memory_space_constraint(total, pltpu.VMEM),
        )
        return first.T, second.T

    placed = (P("batch", "group"), P("batch", "group"))
    return jax.shard_map(
        shards,
        mesh=mesh,
        in_specs=placed,
        out_specs=(P(None, ("group", "batch")), P(None, ("group", "batch"))),
        check_vma=False,
    )
```

```python
import functools

import jax
import jax.numpy as jnp
from jax import lax
from jax.experimental import pallas as pl
from jax.experimental.pallas import tpu as pltpu
from jax.sharding import PartitionSpec as P

MESH = pl.DeviceIdType.MESH
LANES = 128


def loop(count, body, init):
    if count <= 8:
        for step in range(count):
            init = body(step, init)
        return init
    return lax.fori_loop(0, count, body, init)


def kernel(n, first_hbm, second_hbm, got, total, raw, turned, load_sem, send_sem, recv_sem, here):
    ins = (first_hbm, second_hbm)
    rows, width = first_hbm.shape
    block = width // n
    half, quarter = n // 2, n // 4
    span = half * block
    me = lax.axis_index("batch")

    def load(side, a):
        return pltpu.make_async_copy(
            ins[a].at[:, side * span : (side + 1) * span], raw.at[a, side], load_sem.at[a, side]
        )

    for side in range(2):
        for a in range(2):
            load(side, a).start()

    barrier = pltpu.get_barrier_semaphore()

    def greet(target, carry):
        pl.semaphore_signal(
            barrier, inc=1, device_id={"batch": target}, device_id_type=MESH
        )
        return carry

    lax.fori_loop(me + 1, n, greet, 0)

    def send(a, target):
        return pltpu.make_async_remote_copy(
            src_ref=turned.at[a, target],
            dst_ref=got.at[a, me],
            send_sem=send_sem.at[a, target],
            recv_sem=recv_sem.at[a, me],
            device_id={"batch": target},
            device_id_type=MESH,
        )

    def arrival(a, source):
        return pltpu.make_async_remote_copy(
            src_ref=turned.at[a, source],
            dst_ref=got.at[a, source],
            send_sem=send_sem.at[a, source],
            recv_sem=recv_sem.at[a, source],
            device_id={"batch": source},
            device_id_type=MESH,
        )

    def transpose(side, a):
        load(side, a).wait()
        for start in range(0, span, LANES):
            tile = raw[a, side, :, start : start + LANES].T
            spot = side * half + start // block
            turned[a, spot : spot + LANES // block] = tile.reshape(LANES // block, block, rows)

    def push(a, first):
        def one(step, carry):
            target = first + step

            @pl.when(target != me)
            def _():
                if a == 0:

                    @pl.when(target > me)
                    def _():
                        pl.semaphore_wait(here.at[target], 1)

                send(a, target).start()

            return carry

        loop(quarter, one, 0)

    transpose(0, 0)

    @pl.when(me > 0)
    def _():
        pl.semaphore_wait(barrier, me)

    def announce(target, carry):
        pl.semaphore_signal(
            here.at[me], inc=1, device_id={"batch": target}, device_id_type=MESH
        )
        return carry

    lax.fori_loop(0, me, announce, 0)
    push(0, 0)
    transpose(0, 1)
    push(1, 0)
    push(0, quarter)
    push(1, quarter)
    transpose(1, 0)
    transpose(1, 1)
    for first in (half, half + quarter):
        push(0, first)
        push(1, first)

    def add(sums, values):
        low, high = sums
        for start in range(0, rows, LANES):
            part = values[:, start : start + LANES]
            low += jnp.minimum(part, 1.0)
            high += jnp.maximum(part, 1.0)
        return low, high

    zero = jnp.zeros((block, LANES), jnp.float32)
    for a in range(2):
        got[a, me] = turned[a, me]

    def take(source, sums):
        @pl.when(source != me)
        def _():
            for a in range(2):
                arrival(a, source).wait_recv()

        return tuple(add(sums[a], got[a, source]) for a in range(2))

    sums = loop(n, take, ((zero, zero), (zero, zero)))
    for a in range(2):
        for kind in range(2):
            total[a, kind] = sums[a][kind]

    def drain(target, carry):
        @pl.when(target != me)
        def _():
            for a in range(2):
                send(a, target).wait_send()

        return carry

    loop(n, drain, 0)


def rescale(got, total, first_out, second_out, ready, store_sem):
    _, n, block, rows = got.shape
    outs = (first_out, second_out)
    pieces = min(n, 4)
    each = n // pieces
    copies = []
    for a in range(2):
        low, high = (
            jnp.sum(total[a, kind], axis=1, keepdims=True) / (n * rows) for kind in range(2)
        )
        scale = 1.0 / (high - low + 0.1)
        low = jnp.broadcast_to(low, (block, rows))
        scale = jnp.broadcast_to(scale, (block, rows))
        for piece in range(pieces):

            def turn(step, carry, a=a, piece=piece, low=low, scale=scale):
                source = piece * each + step
                start = source * rows
                if not isinstance(start, int):
                    start = pl.multiple_of(start, LANES)
                ready[a, :, pl.ds(start, rows)] = (got[a, source] - low) * scale
                return carry

            loop(each, turn, 0)
            part = pl.ds(piece * each * rows, each * rows)
            copy = pltpu.make_async_copy(
                ready.at[a, :, part], outs[a].at[:, part], store_sem.at[a, piece]
            )
            copy.start()
            copies.append(copy)
    for copy in copies:
        copy.wait()


def solution(mesh):
    n = mesh.shape["batch"]

    def shards(samples_in, second_samples_in):
        rows, width = samples_in.shape
        block = width // n
        half = n // 2
        held = 2 * rows * width * 4
        got, total = pl.pallas_call(
            functools.partial(kernel, n),
            out_shape=(
                pltpu.VMEM((2, n, block, rows), jnp.float32),
                pltpu.VMEM((2, 2, block, LANES), jnp.float32),
            ),
            in_specs=[pl.BlockSpec(memory_space=pltpu.HBM)] * 2,
            out_specs=[pl.BlockSpec(memory_space=pltpu.VMEM)] * 2,
            scratch_shapes=[
                pltpu.VMEM((2, 2, rows, half * block), jnp.float32),
                pltpu.VMEM((2, n, block, rows), jnp.float32),
                pltpu.SemaphoreType.DMA((2, 2)),
                pltpu.SemaphoreType.DMA((2, n)),
                pltpu.SemaphoreType.DMA((2, n)),
                pltpu.SemaphoreType.REGULAR((n,)),
            ],
            compiler_params=pltpu.CompilerParams(
                collective_id=0, has_side_effects=True, vmem_limit_bytes=4 * held + (8 << 20)
            ),
            name="exchange",
        )(
            pltpu.with_memory_space_constraint(samples_in, pltpu.HBM),
            pltpu.with_memory_space_constraint(second_samples_in, pltpu.HBM),
        )
        out = jax.ShapeDtypeStruct((block, n * rows), jnp.float32)
        first, second = pl.pallas_call(
            rescale,
            out_shape=(out, out),
            in_specs=[pl.BlockSpec(memory_space=pltpu.VMEM)] * 2,
            out_specs=[pl.BlockSpec(memory_space=pl.ANY)] * 2,
            scratch_shapes=[
                pltpu.VMEM((2, block, n * rows), jnp.float32),
                pltpu.SemaphoreType.DMA((2, min(n, 4))),
            ],
            compiler_params=pltpu.CompilerParams(vmem_limit_bytes=2 * held + (8 << 20)),
            name="rescale",
        )(
            pltpu.with_memory_space_constraint(got, pltpu.VMEM),
            pltpu.with_memory_space_constraint(total, pltpu.VMEM),
        )
        return first.T, second.T

    placed = (P("batch", "group"), P("batch", "group"))
    return jax.shard_map(
        shards,
        mesh=mesh,
        in_specs=placed,
        out_specs=(P(None, ("group", "batch")), P(None, ("group", "batch"))),
        check_vma=False,
    )
```

```python
import functools

import jax
import jax.numpy as jnp
from jax import lax
from jax.experimental import pallas as pl
from jax.experimental.pallas import tpu as pltpu
from jax.sharding import PartitionSpec as P

MESH = pl.DeviceIdType.MESH
LANES = 128


def loop(count, body, init):
    if count <= 8:
        for step in range(count):
            init = body(step, init)
        return init
    return lax.fori_loop(0, count, body, init)


def kernel(n, first_hbm, second_hbm, got, total, raw, turned, load_sem, send_sem, recv_sem, here):
    ins = (first_hbm, second_hbm)
    rows, width = first_hbm.shape
    block = width // n
    half, quarter = n // 2, n // 4
    span = half * block
    me = lax.axis_index("batch")

    def load(side, a):
        return pltpu.make_async_copy(
            ins[a].at[:, side * span : (side + 1) * span], raw.at[a, side], load_sem.at[a, side]
        )

    for side in range(2):
        for a in range(2):
            load(side, a).start()

    barrier = pltpu.get_barrier_semaphore()

    def greet(target, carry):
        pl.semaphore_signal(
            barrier, inc=1, device_id={"batch": target}, device_id_type=MESH
        )
        return carry

    lax.fori_loop(me + 1, n, greet, 0)

    def send(a, target):
        return pltpu.make_async_remote_copy(
            src_ref=turned.at[a, target],
            dst_ref=got.at[a, me],
            send_sem=send_sem.at[a, target],
            recv_sem=recv_sem.at[a, me],
            device_id={"batch": target},
            device_id_type=MESH,
        )

    def arrival(a, source):
        return pltpu.make_async_remote_copy(
            src_ref=turned.at[a, source],
            dst_ref=got.at[a, source],
            send_sem=send_sem.at[a, source],
            recv_sem=recv_sem.at[a, source],
            device_id={"batch": source},
            device_id_type=MESH,
        )

    def transpose(side, a):
        load(side, a).wait()
        for start in range(0, span, LANES):
            tile = raw[a, side, :, start : start + LANES].T
            spot = side * half + start // block
            turned[a, spot : spot + LANES // block] = tile.reshape(LANES // block, block, rows)

    def push(a, first, count):
        def one(step, carry):
            target = first + step

            @pl.when(target != me)
            def _():
                if a == 0:

                    @pl.when(target > me)
                    def _():
                        pl.semaphore_wait(here.at[target], 1)

                send(a, target).start()

            return carry

        loop(count, one, 0)


    @pl.when(me > 0)
    def _():
        pl.semaphore_wait(barrier, me)

    def announce(target, carry):
        pl.semaphore_signal(
            here.at[me], inc=1, device_id={"batch": target}, device_id_type=MESH
        )
        return carry

    lax.fori_loop(0, me, announce, 0)
    transpose(0, 0)
    transpose(0, 1)
    push(0, 0, 1)
    push(1, 0, 1)
    push(0, 1, quarter - 1)
    push(1, 1, quarter - 1)
    push(0, quarter, quarter)
    push(1, quarter, quarter)
    transpose(1, 0)
    transpose(1, 1)
    for first in (half, half + quarter):
        push(0, first, quarter)
        push(1, first, quarter)

    def add(sums, values):
        low, high = sums
        for start in range(0, rows, LANES):
            part = values[:, start : start + LANES]
            low += jnp.minimum(part, 1.0)
            high += jnp.maximum(part, 1.0)
        return low, high

    zero = jnp.zeros((block, LANES), jnp.float32)
    for a in range(2):
        got[a, me] = turned[a, me]

    def take(source, sums):
        @pl.when(source != me)
        def _():
            for a in range(2):
                arrival(a, source).wait_recv()

        return tuple(add(sums[a], got[a, source]) for a in range(2))

    sums = loop(n, take, ((zero, zero), (zero, zero)))
    for a in range(2):
        for kind in range(2):
            total[a, kind] = sums[a][kind]

    def drain(target, carry):
        @pl.when(target != me)
        def _():
            for a in range(2):
                send(a, target).wait_send()

        return carry

    loop(n, drain, 0)


def rescale(got, total, first_out, second_out, ready, store_sem):
    _, n, block, rows = got.shape
    outs = (first_out, second_out)
    pieces = min(n, 4)
    each = n // pieces
    copies = []
    for a in range(2):
        low, high = (
            jnp.sum(total[a, kind], axis=1, keepdims=True) / (n * rows) for kind in range(2)
        )
        scale = 1.0 / (high - low + 0.1)
        low = jnp.broadcast_to(low, (block, rows))
        scale = jnp.broadcast_to(scale, (block, rows))
        for piece in range(pieces):

            def turn(step, carry, a=a, piece=piece, low=low, scale=scale):
                source = piece * each + step
                start = source * rows
                if not isinstance(start, int):
                    start = pl.multiple_of(start, LANES)
                ready[a, :, pl.ds(start, rows)] = (got[a, source] - low) * scale
                return carry

            loop(each, turn, 0)
            part = pl.ds(piece * each * rows, each * rows)
            copy = pltpu.make_async_copy(
                ready.at[a, :, part], outs[a].at[:, part], store_sem.at[a, piece]
            )
            copy.start()
            copies.append(copy)
    for copy in copies:
        copy.wait()


def solution(mesh):
    n = mesh.shape["batch"]

    def shards(samples_in, second_samples_in):
        rows, width = samples_in.shape
        block = width // n
        half = n // 2
        held = 2 * rows * width * 4
        got, total = pl.pallas_call(
            functools.partial(kernel, n),
            out_shape=(
                pltpu.VMEM((2, n, block, rows), jnp.float32),
                pltpu.VMEM((2, 2, block, LANES), jnp.float32),
            ),
            in_specs=[pl.BlockSpec(memory_space=pltpu.HBM)] * 2,
            out_specs=[pl.BlockSpec(memory_space=pltpu.VMEM)] * 2,
            scratch_shapes=[
                pltpu.VMEM((2, 2, rows, half * block), jnp.float32),
                pltpu.VMEM((2, n, block, rows), jnp.float32),
                pltpu.SemaphoreType.DMA((2, 2)),
                pltpu.SemaphoreType.DMA((2, n)),
                pltpu.SemaphoreType.DMA((2, n)),
                pltpu.SemaphoreType.REGULAR((n,)),
            ],
            compiler_params=pltpu.CompilerParams(
                collective_id=0, has_side_effects=True, vmem_limit_bytes=4 * held + (8 << 20)
            ),
            name="exchange",
        )(
            pltpu.with_memory_space_constraint(samples_in, pltpu.HBM),
            pltpu.with_memory_space_constraint(second_samples_in, pltpu.HBM),
        )
        out = jax.ShapeDtypeStruct((block, n * rows), jnp.float32)
        first, second = pl.pallas_call(
            rescale,
            out_shape=(out, out),
            in_specs=[pl.BlockSpec(memory_space=pltpu.VMEM)] * 2,
            out_specs=[pl.BlockSpec(memory_space=pl.ANY)] * 2,
            scratch_shapes=[
                pltpu.VMEM((2, block, n * rows), jnp.float32),
                pltpu.SemaphoreType.DMA((2, min(n, 4))),
            ],
            compiler_params=pltpu.CompilerParams(vmem_limit_bytes=2 * held + (8 << 20)),
            name="rescale",
        )(
            pltpu.with_memory_space_constraint(got, pltpu.VMEM),
            pltpu.with_memory_space_constraint(total, pltpu.VMEM),
        )
        return first.T, second.T

    placed = (P("batch", "group"), P("batch", "group"))
    return jax.shard_map(
        shards,
        mesh=mesh,
        in_specs=placed,
        out_specs=(P(None, ("group", "batch")), P(None, ("group", "batch"))),
        check_vma=False,
    )
```

```python
import functools

import jax
import jax.numpy as jnp
from jax import lax
from jax.experimental import pallas as pl
from jax.experimental.pallas import tpu as pltpu
from jax.sharding import PartitionSpec as P

MESH = pl.DeviceIdType.MESH
LANES = 128


def loop(count, body, init):
    if count <= 8:
        for step in range(count):
            init = body(step, init)
        return init
    return lax.fori_loop(0, count, body, init)


def kernel(n, first_hbm, second_hbm, got, total, raw, turned, load_sem, send_sem, recv_sem, here):
    ins = (first_hbm, second_hbm)
    rows, width = first_hbm.shape
    block = width // n
    half = n // 2
    span = half * block
    me = lax.axis_index("batch")

    def load(side, a):
        return pltpu.make_async_copy(
            ins[a].at[:, side * span : (side + 1) * span], raw.at[a, side], load_sem.at[a, side]
        )

    for side in range(2):
        for a in range(2):
            load(side, a).start()

    barrier = pltpu.get_barrier_semaphore()

    def greet(target, carry):
        pl.semaphore_signal(
            barrier, inc=1, device_id={"batch": target}, device_id_type=MESH
        )
        return carry

    lax.fori_loop(me + 1, n, greet, 0)

    def send(a, target):
        return pltpu.make_async_remote_copy(
            src_ref=turned.at[a, target],
            dst_ref=got.at[a, me],
            send_sem=send_sem.at[a, target],
            recv_sem=recv_sem.at[a, me],
            device_id={"batch": target},
            device_id_type=MESH,
        )

    def arrival(a, source):
        return pltpu.make_async_remote_copy(
            src_ref=turned.at[a, source],
            dst_ref=got.at[a, source],
            send_sem=send_sem.at[a, source],
            recv_sem=recv_sem.at[a, source],
            device_id={"batch": source},
            device_id_type=MESH,
        )

    def transpose(side, a):
        load(side, a).wait()
        for start in range(0, span, LANES):
            tile = raw[a, side, :, start : start + LANES].T
            spot = side * half + start // block
            turned[a, spot : spot + LANES // block] = tile.reshape(LANES // block, block, rows)

    def push(first, count):
        def one(step, carry):
            target = first + step

            @pl.when(target > me)
            def _():
                pl.semaphore_wait(here.at[target], 1)

            @pl.when(target != me)
            def _():
                for a in range(2):
                    send(a, target).start()

            return carry

        loop(count, one, 0)

    @pl.when(me > 0)
    def _():
        pl.semaphore_wait(barrier, me)

    def announce(target, carry):
        pl.semaphore_signal(
            here.at[me], inc=1, device_id={"batch": target}, device_id_type=MESH
        )
        return carry

    lax.fori_loop(0, me, announce, 0)
    transpose(0, 0)
    transpose(0, 1)
    push(0, half)
    transpose(1, 0)
    transpose(1, 1)
    push(half, half)

    def add(sums, values):
        low, high = sums
        for start in range(0, rows, LANES):
            part = values[:, start : start + LANES]
            low += jnp.minimum(part, 1.0)
            high += jnp.maximum(part, 1.0)
        return low, high

    zero = jnp.zeros((block, LANES), jnp.float32)
    for a in range(2):
        got[a, me] = turned[a, me]

    def take(source, sums):
        @pl.when(source != me)
        def _():
            for a in range(2):
                arrival(a, source).wait_recv()

        return tuple(add(sums[a], got[a, source]) for a in range(2))

    sums = loop(n, take, ((zero, zero), (zero, zero)))
    for a in range(2):
        for kind in range(2):
            total[a, kind] = sums[a][kind]

    def drain(target, carry):
        @pl.when(target != me)
        def _():
            for a in range(2):
                send(a, target).wait_send()

        return carry

    loop(n, drain, 0)


def rescale(got, total, first_out, second_out, ready, store_sem):
    _, n, block, rows = got.shape
    outs = (first_out, second_out)
    pieces = min(n, 4)
    each = n // pieces
    copies = []
    for a in range(2):
        low, high = (
            jnp.sum(total[a, kind], axis=1, keepdims=True) / (n * rows) for kind in range(2)
        )
        scale = 1.0 / (high - low + 0.1)
        low = jnp.broadcast_to(low, (block, rows))
        scale = jnp.broadcast_to(scale, (block, rows))
        for piece in range(pieces):

            def turn(step, carry, a=a, piece=piece, low=low, scale=scale):
                source = piece * each + step
                start = source * rows
                if not isinstance(start, int):
                    start = pl.multiple_of(start, LANES)
                ready[a, :, pl.ds(start, rows)] = (got[a, source] - low) * scale
                return carry

            loop(each, turn, 0)
            part = pl.ds(piece * each * rows, each * rows)
            copy = pltpu.make_async_copy(
                ready.at[a, :, part], outs[a].at[:, part], store_sem.at[a, piece]
            )
            copy.start()
            copies.append(copy)
    for copy in copies:
        copy.wait()


def solution(mesh):
    n = mesh.shape["batch"]

    def shards(samples_in, second_samples_in):
        rows, width = samples_in.shape
        block = width // n
        half = n // 2
        held = 2 * rows * width * 4
        got, total = pl.pallas_call(
            functools.partial(kernel, n),
            out_shape=(
                pltpu.VMEM((2, n, block, rows), jnp.float32),
                pltpu.VMEM((2, 2, block, LANES), jnp.float32),
            ),
            in_specs=[pl.BlockSpec(memory_space=pltpu.HBM)] * 2,
            out_specs=[pl.BlockSpec(memory_space=pltpu.VMEM)] * 2,
            scratch_shapes=[
                pltpu.VMEM((2, 2, rows, half * block), jnp.float32),
                pltpu.VMEM((2, n, block, rows), jnp.float32),
                pltpu.SemaphoreType.DMA((2, 2)),
                pltpu.SemaphoreType.DMA((2, n)),
                pltpu.SemaphoreType.DMA((2, n)),
                pltpu.SemaphoreType.REGULAR((n,)),
            ],
            compiler_params=pltpu.CompilerParams(
                collective_id=0, has_side_effects=True, vmem_limit_bytes=4 * held + (8 << 20)
            ),
            name="exchange",
        )(
            pltpu.with_memory_space_constraint(samples_in, pltpu.HBM),
            pltpu.with_memory_space_constraint(second_samples_in, pltpu.HBM),
        )
        out = jax.ShapeDtypeStruct((block, n * rows), jnp.float32)
        first, second = pl.pallas_call(
            rescale,
            out_shape=(out, out),
            in_specs=[pl.BlockSpec(memory_space=pltpu.VMEM)] * 2,
            out_specs=[pl.BlockSpec(memory_space=pl.ANY)] * 2,
            scratch_shapes=[
                pltpu.VMEM((2, block, n * rows), jnp.float32),
                pltpu.SemaphoreType.DMA((2, min(n, 4))),
            ],
            compiler_params=pltpu.CompilerParams(vmem_limit_bytes=2 * held + (8 << 20)),
            name="rescale",
        )(
            pltpu.with_memory_space_constraint(got, pltpu.VMEM),
            pltpu.with_memory_space_constraint(total, pltpu.VMEM),
        )
        return first.T, second.T

    placed = (P("batch", "group"), P("batch", "group"))
    return jax.shard_map(
        shards,
        mesh=mesh,
        in_specs=placed,
        out_specs=(P(None, ("group", "batch")), P(None, ("group", "batch"))),
        check_vma=False,
    )
```
